32 devices in a mesh: probe: 4 (over y, x), space: 8 (over z, core).
Axes of the slice: x: 2, y: 2, z: 4, core: 2. Of those that a mesh axis runs over, the one named last changes fastest.
Arguments:
- probe_signs: int32 [192, 64, 1024], P('probe', 'space'), may hold values from 0 to 1, as said below
- sensor_mask: int32 [64, 1024], P('space'), may hold values 0 or 1
- sensor_weight: float32 [64, 1024], P('space'), may hold values from 1 to 30
- prior_mass: float32 [64, 1024], P('space'), may hold values from 0.02 to 0.5
Outputs:
- solution: float32 [192, 64, 1024], P('probe', 'space')
- trace_cell: float32 [], replicated
The draws below stay inside these ranges and needn't reach their ends.
Inputs may be any that keep to these rules, and one draw needn't show every extreme that they name: `probe_signs`: each entry is 0 or 1; the probe's sign is twice the entry minus one.
All inputs are finite; a program needn't handle non-finite values. No bound on the sum of `sensor_mask` on one device may be relied on, other than what follows from the above.
Results may differ from the reference program's by a relative error of at most 0.0001.
Values sent between devices are 32-bit elements; how exact they have to be, the bound alone decides.
A program may use at most 64 MiB of HBM per device.

```python
import math
import jax
import jax.numpy as jnp
from jax import lax

PROBES_DEV = 48
ITERS = 4
NX = 64
NY = 1024
PROBES = 192


def draw_probe_signs(key, part):
    levels = 1048576
    probe_index = jnp.arange(PROBES, dtype=jnp.int32)
    threshold = 524288 + 471859 * probe_index // max(PROBES - 1, 1)
    uniform_bits = jax.random.randint(jax.random.fold_in(key, 17), (PROBES, NX, NY), 0, levels, dtype=jnp.int32)
    return (uniform_bits < threshold[:, None, None]).astype(jnp.int32)


def place_ends(drawn, stream_key, low, high):
    spot = [jax.random.randint(jax.random.fold_in(stream_key, axis), (), 0, length) for axis, length in enumerate(drawn.shape)]
    widest = drawn.shape.index(max(drawn.shape))
    neighbour = spot[:widest] + [(spot[widest] + 1) % drawn.shape[widest]] + spot[widest + 1:]
    return drawn.at[tuple(spot)].set(low).at[tuple(neighbour)].set(high)


def shard_levels(stream_key, dims, pieces, low, top_value):
    level, own = 1.0, jax.random.fold_in(stream_key, 6)
    for axis_at, blocks in pieces:
        steps = jnp.exp(jax.random.uniform(jax.random.fold_in(own, axis_at), (blocks,), jnp.float32, low / len(pieces), top_value / len(pieces)))
        level = level * jnp.repeat(steps, dims[axis_at] // blocks).reshape([-1 if axis == axis_at else 1 for axis in range(len(dims))])
    return level


def setup_inputs(seed: int = 0) -> dict:
    arg_keys = jax.random.split(jax.random.key(seed), 5)
    probe_signs = draw_probe_signs(jax.random.fold_in(arg_keys[4], 71), 0)
    sensor_mask = place_ends((jax.random.randint(arg_keys[1], (NX, NY), 0, 8) < 1).astype(jnp.int32), jax.random.fold_in(arg_keys[1], 1), 0, 1)
    sensor_weight = jnp.clip(jnp.exp(math.log(30.0) - 3.4011974 * jax.random.uniform(arg_keys[2], (NX, NY), jnp.float32) ** shard_levels(arg_keys[2], (NX, NY), ((0, 8),), -0.2, 0.2)), 1.0, 30.0)
    prior_mass = jnp.clip(jnp.exp(math.log(0.5) - 3.218876 * jax.random.uniform(arg_keys[3], (NX, NY), jnp.float32) ** shard_levels(arg_keys[3], (NX, NY), ((0, 8),), -0.2, 0.2)), 0.02, 0.5)
    return {"probe_signs": probe_signs, "sensor_mask": sensor_mask, "sensor_weight": sensor_weight, "prior_mass": prior_mass}


def operate(vector_in, diagonal):
    padded = jnp.pad(vector_in, ((0, 0), (1, 1), (1, 1)))
    beside = padded[:, 2:, 1:-1] + padded[:, :-2, 1:-1]
    beside = beside + padded[:, 1:-1, 2:] + padded[:, 1:-1, :-2]
    return (4.0 + diagonal) * vector_in - beside


def solve_block(probe_block, diagonal):
    probes = 2.0 * probe_block.astype(jnp.float32) - 1.0
    solution = jnp.zeros_like(probes)
    residual = probes
    direction = probes
    norm_now = jnp.sum(residual * residual, axis=(1, 2))
    for iterate in range(ITERS):
        applied = operate(direction, diagonal)
        step_len = norm_now / jnp.sum(direction * applied, axis=(1, 2))
        solution = solution + step_len[:, None, None] * direction
        residual = residual - step_len[:, None, None] * applied
        norm_next = jnp.sum(residual * residual, axis=(1, 2))
        direction = residual + (norm_next / norm_now)[:, None, None] * direction
        norm_now = norm_next
    return solution, jnp.sum(probes * solution)


def reference(probe_signs, sensor_mask, sensor_weight, prior_mass):
    diagonal = sensor_mask.astype(jnp.float32) * sensor_weight + prior_mass
    blocks = probe_signs.reshape(PROBES // PROBES_DEV, PROBES_DEV, NX, NY)

    def one_block(probe_block):
        return solve_block(probe_block, diagonal)

    solutions, partial_sums = lax.map(one_block, blocks)
    solution = solutions.reshape(PROBES, NX, NY)
    trace_cell = jnp.sum(partial_sums) / float(PROBES * NX * NY)
    return solution, trace_cell
```

```python
import functools

import jax
import jax.numpy as jnp
from jax import lax
from jax.experimental import pallas as pl
from jax.experimental.pallas import tpu as pltpu
from jax.sharding import PartitionSpec as P

MESH = pl.DeviceIdType.MESH
LANES = 128
SHIFT = 4.0
LOW = 0.02
TINY = 1e-30


def split(block):
    return [block[:, t * LANES : (t + 1) * LANES] for t in range(block.shape[1] // LANES)]


def sideways(tiles, lane):
    ahead = [pltpu.roll(v, 1, 1) for v in tiles]
    behind = [pltpu.roll(v, LANES - 1, 1) for v in tiles]
    zero = jnp.zeros_like(tiles[0])
    count = len(tiles)
    out = []
    for t in range(count):
        west = jnp.where(lane == 0, ahead[t - 1] if t else zero, ahead[t])
        east = jnp.where(lane == LANES - 1, behind[t + 1] if t + 1 < count else zero, behind[t])
        out.append(west + east)
    return out


def upright(own, halo, row, want_own, want_halo):
    rows = own[0].shape[0]
    for_own, for_halo = [], []
    for o, h in zip(own, halo):
        o_down, h_down = pltpu.roll(o, 1, 0), pltpu.roll(h, 1, 0)
        o_up, h_up = pltpu.roll(o, rows - 1, 0), pltpu.roll(h, rows - 1, 0)
        if want_own:
            for_own.append(jnp.where(row == 0, h_down, o_down) + jnp.where(row == rows - 1, h_up, o_up))
        if want_halo:
            for_halo.append(jnp.where(row == 0, o_down, h_down) + jnp.where(row == rows - 1, o_up, h_up))
    return for_own, for_halo


def apply_own(own, halo, diag, lane, row):
    up, _ = upright(own, halo, row, True, False)
    side = sideways(own, lane)
    return [d * v - (u + s) for d, v, u, s in zip(diag, own, up, side)]


def apply_halo(own, halo, diag, mask, lane, row):
    _, up = upright(own, halo, row, False, True)
    side = sideways(halo, lane)
    return [d * v - mask * (u + s) for d, v, u, s in zip(diag, halo, up, side)]


def apply_both(own, halo, diag, diag_h, mask, lane, row):
    up, up_h = upright(own, halo, row, True, True)
    side, side_h = sideways(own, lane), sideways(halo, lane)
    return (
        [d * v - (u + s) for d, v, u, s in zip(diag, own, up, side)],
        [d * v - mask * (u + s) for d, v, u, s in zip(diag_h, halo, up_h, side_h)],
    )


def dot(left, right):
    total = left[0] * right[0]
    for a, b in zip(left[1:], right[1:]):
        total = total + a * b
    return jnp.sum(total, axis=0, keepdims=True)


def first_steps(m1, m2, m3, m4):
    sigma = SHIFT
    a0 = sigma + m1
    b1 = jnp.maximum(m2 - m1 * m1, 0.0)
    h3 = m3 - 2.0 * m1 * m2 + m1 * m1 * m1
    s0 = 1.0 / jnp.maximum(a0, LOW)
    rr1 = s0 * s0 * b1
    pq1 = s0 * s0 * (h3 + sigma * b1) - rr1 * rr1 / s0
    s1 = rr1 / jnp.maximum(jnp.maximum(pq1, LOW * rr1), TINY)
    p1b, p1g = s0 * m1 + rr1, -s0
    r2b = s0 * m1 - s1 * sigma * p1b
    r2g = -s0 - s1 * (sigma * p1g + p1b)
    r2y = -s1 * p1g
    rr2 = jnp.maximum(r2y * (r2b * m2 + r2g * m3 + r2y * m4), 0.0)
    be1 = rr2 / jnp.maximum(rr1, TINY)
    p2b, p2g, p2y = r2b + be1 * p1b, r2g + be1 * p1g, r2y
    return dict(s0=s0, s1=s1, p1b=p1b, p1g=p1g, pq1=pq1, be1=be1, r2=(r2b, r2g, r2y), p2=(p2b, p2g, p2y))


def last_steps(st, sums):
    rr, rp, pp, pq, rq, qq, rw, qw = sums
    sigma = SHIFT
    full_pq = pq + sigma * pp
    s2 = rr / jnp.maximum(jnp.maximum(full_pq, LOW * rr), TINY)
    full_rq = rq + sigma * rp
    full_qq = qq + 2.0 * sigma * pq + sigma * sigma * pp
    rr3 = jnp.maximum(rr - 2.0 * s2 * full_rq + s2 * s2 * full_qq, 0.0)
    be2 = rr3 / jnp.maximum(rr, TINY)
    rhr2 = full_pq + st["be1"] * st["be1"] * st["pq1"]
    rhq = rw + 2.0 * sigma * rq + sigma * sigma * rp
    qhq = qw + 3.0 * sigma * qq + 3.0 * sigma * sigma * pq + sigma * sigma * sigma * pp
    rhr3 = rhr2 - 2.0 * s2 * rhq + s2 * s2 * qhq
    pq3 = rhr3 - rr3 * rr3 / jnp.maximum(rr * s2, TINY)
    s3 = rr3 / jnp.maximum(jnp.maximum(pq3, LOW * rr3), TINY)
    cp, cr, cq = s2 + s3 * (be2 - s2 * sigma), s3, -s3 * s2
    r2, p2 = st["r2"], st["p2"]
    xb = st["s0"] + st["s1"] * st["p1b"] + cp * p2[0] + cr * r2[0]
    xg = st["s1"] * st["p1g"] + cp * p2[1] + cr * r2[1]
    xy = cp * p2[2] + cr * r2[2]
    return xb, xg, xy, cq


def kernel(
    names, chunk, signs_hbm, mask_ref, weight_ref, prior_ref, out_hbm, trace_ref,
    signs, halo, halo_far, diag, diag_h, g_own, g_halo, y_own, y_halo, q_own, x_own,
    acc, mine, parts, tr_mine, tr_parts, coef,
    load_sem, out_sem, dsend, drecv, hsend, hrecv, ssend, srecv, tsend, trecv,
):
    probe_axis, space_axis = names
    probe, space = lax.axis_index(probe_axis), lax.axis_index(space_axis)
    probe_n, space_n = lax.axis_size(probe_axis), lax.axis_size(space_axis)
    probes, rows, cols = signs.shape
    half = rows // 2
    quarter = half // 2
    chunks = probes // chunk
    cells = float(rows * space_n * cols)

    barrier = pltpu.get_barrier_semaphore()
    for k in range(1, space_n):
        pl.semaphore_signal(barrier, 1, device_id=(probe, lax.rem(space + k, space_n)), device_id_type=MESH)
    for k in range(1, probe_n):
        pl.semaphore_signal(barrier, 1, device_id=(lax.rem(probe + k, probe_n), space), device_id_type=MESH)
    loads = pltpu.make_async_copy(signs_hbm, signs, load_sem)
    loads.start()
    diag[...] = mask_ref[...].astype(jnp.float32) * weight_ref[...] + prior_ref[...]
    loads.wait()
    pl.semaphore_wait(barrier, space_n + probe_n - 2)

    has_prev, has_next = space > 0, space < space_n - 1
    prev, nxt = (probe, jnp.maximum(space - 1, 0)), (probe, jnp.minimum(space + 1, space_n - 1))

    def pieces(stage):
        if stage == 0:
            return (0, quarter), (rows - quarter, quarter)
        return (quarter, half - quarter), (half, half - quarter)

    def halo_copy(stage, c, side):
        start, size = pieces(stage)[side]
        at = (pl.ds(c * chunk, chunk), pl.ds(start, size))
        return pltpu.make_async_remote_copy(
            src_ref=signs.at[at], dst_ref=(halo, halo_far)[stage].at[at],
            send_sem=hsend.at[stage, side, c], recv_sem=hrecv.at[stage, side, c],
            device_id=(prev, nxt)[side], device_id_type=MESH,
        )

    def diag_copy(side):
        at = pl.ds(side * half, half)
        return pltpu.make_async_remote_copy(
            src_ref=diag.at[at], dst_ref=diag_h.at[at],
            send_sem=dsend.at[side], recv_sem=drecv.at[side],
            device_id=(prev, nxt)[side], device_id_type=MESH,
        )

    for side, there in ((0, has_prev), (1, has_next)):
        @pl.when(there)
        def _():
            diag_copy(side).start()
    for stage in (0, 1):
        for c in range(chunks):
            for side, there in ((0, has_prev), (1, has_next)):
                @pl.when(there)
                def _():
                    halo_copy(stage, c, side).start()

    for side, there in ((0, has_next), (1, has_prev)):
        @pl.when(there)
        def _():
            diag_copy(side).wait_recv()

    row = lax.broadcasted_iota(jnp.int32, (rows, LANES), 0)
    lane = lax.broadcasted_iota(jnp.int32, (rows, LANES), 1)
    below = jnp.where(has_next, 1.0, 0.0)
    above = jnp.where(has_prev, 1.0, 0.0)
    mask = jnp.where(row < half, below, above)
    live = mask > 0.5
    wide = lax.broadcasted_iota(jnp.int32, (rows, cols), 0)
    diag_h[...] = jnp.where(jnp.where(wide < half, below, above) > 0.5, diag_h[...], 0.0)

    def field(ref, p):
        return split(2.0 * ref[p].astype(jnp.float32) - 1.0)

    near = (row < quarter) | (row >= rows - quarter)

    def near_field(p):
        return [jnp.where(live & near, v, 0.0) for v in field(halo, p)]

    def halo_field(p):
        pairs = zip(split(halo[p]), split(halo_far[p]))
        return [jnp.where(live, 2.0 * jnp.where(near, a, b).astype(jnp.float32) - 1.0, 0.0) for a, b in pairs]

    def keep(ref, p, tiles):
        for t, v in enumerate(tiles):
            ref[p, :, t * LANES : (t + 1) * LANES] = v

    def first(p, carry):
        own, out = field(signs, p), near_field(p)
        d, dh = split(diag[...]), split(diag_h[...])
        g, gh = apply_both(own, out, d, dh, mask, lane, row)
        y = apply_own(g, gh, d, lane, row)
        keep(g_own, p, g)
        keep(y_own, p, y)
        for k, (a, b) in enumerate(((own, g), (g, g), (g, y), (y, y))):
            acc[k, pl.ds(p, 1), :] = dot(a, b)
        return carry

    def second(p, carry):
        own, out = field(signs, p), halo_field(p)
        dh = split(diag_h[...])
        g = split(g_own[p])
        gh = apply_halo(own, out, dh, mask, lane, row)
        yh = apply_halo(g, gh, dh, mask, lane, row)
        keep(g_halo, p, gh)
        keep(y_halo, p, yh)
        return carry

    def await_halo(stage, c):
        for side, there in ((0, has_next), (1, has_prev)):
            @pl.when(there)
            def _():
                halo_copy(stage, c, side).wait_recv()

    for c in range(chunks):
        await_halo(0, c)
        lax.fori_loop(c * chunk, (c + 1) * chunk, first, 0)

    def sum_copy(which, k):
        other = lax.rem(space + k, space_n)
        return pltpu.make_async_remote_copy(
            src_ref=mine.at[which], dst_ref=parts.at[which, k],
            send_sem=ssend.at[which, k], recv_sem=srecv.at[which, k],
            device_id=(probe, other), device_id_type=MESH,
        )

    def send_sums(which, count):
        wide_lane = lax.broadcasted_iota(jnp.int32, (probes, LANES), 1)
        table = jnp.zeros((probes, LANES), jnp.float32)
        for k in range(count):
            table = jnp.where(wide_lane == k, jnp.sum(acc[k], axis=1, keepdims=True), table)
        table = jnp.concatenate([table, jnp.zeros((LANES - probes, LANES), jnp.float32)], axis=0)
        mine[which] = jnp.transpose(table)[:8]
        for k in range(1, space_n):
            sum_copy(which, k).start()

    def take_sums(which):
        for k in range(1, space_n):
            sum_copy(which, k).wait_recv()
        parts[which, 0] = mine[which]
        total = None
        for s in range(space_n):
            part = parts[which, lax.rem(space - s + space_n, space_n)]
            total = part if total is None else total + part
        total = total / cells
        return [total[k : k + 1] for k in range(8)]

    def spread(values):
        r8 = lax.broadcasted_iota(jnp.int32, (8, LANES), 0)
        table = jnp.zeros((8, LANES), jnp.float32)
        for k, v in enumerate(values):
            table = jnp.where(r8 == k, jnp.broadcast_to(v, (8, LANES)), table)
        table = jnp.concatenate([table, jnp.zeros((LANES - 8, LANES), jnp.float32)], axis=0)
        columns = jnp.transpose(table)
        for k in range(len(values)):
            coef[k] = jnp.broadcast_to(columns[:probes, k : k + 1], (probes, LANES))

    def combine(scales, *fields):
        out = []
        for tiles in zip(*fields):
            total = scales[0] * tiles[0]
            for s, v in zip(scales[1:], tiles[1:]):
                total = total + s * v
            out.append(total)
        return out

    def scale(k, p):
        return jnp.broadcast_to(coef[k, pl.ds(p, 1), :], (rows, LANES))

    send_sums(0, 4)
    for c in range(chunks):
        await_halo(1, c)
        lax.fori_loop(c * chunk, (c + 1) * chunk, second, 0)
    m1, m2, m3, m4 = take_sums(0)[:4]
    st = first_steps(m1, m2, m3, m4)
    spread(st["r2"] + st["p2"])

    def third(p, carry):
        own, out = field(signs, p), halo_field(p)
        g, y = split(g_own[p]), split(y_own[p])
        d, dh = split(diag[...]), split(diag_h[...])
        cs = [scale(k, p) for k in range(6)]
        p2 = combine(cs[3:], own, g, y)
        p2h = combine(cs[3:], out, split(g_halo[p]), split(y_halo[p]))
        q, qh = apply_both(p2, p2h, d, dh, mask, lane, row)
        keep(q_own, p, q)
        w = apply_own(q, qh, d, lane, row)
        r2 = combine(cs[:3], own, g, y)
        pairs = ((r2, r2), (r2, p2), (p2, p2), (p2, q), (r2, q), (q, q), (r2, w), (q, w))
        for k, (a, b) in enumerate(pairs):
            acc[k, pl.ds(p, 1), :] = dot(a, b)
        return carry

    lax.fori_loop(0, probes, third, 0)
    send_sums(1, 8)
    xb, xg, xy, cq = last_steps(st, take_sums(1))
    p2 = st["p2"]
    trace = xb + xg * m1 + xy * m2 + cq * (p2[0] * m1 + p2[1] * m2 + p2[2] * m3)
    lane1 = lax.broadcasted_iota(jnp.int32, (1, LANES), 1)
    trace = jnp.where(lane1 < probes, trace, 0.0)
    tr_mine[...] = jnp.broadcast_to(trace, tr_mine.shape)

    def trace_copy(k):
        return pltpu.make_async_remote_copy(
            src_ref=tr_mine, dst_ref=tr_parts.at[k],
            send_sem=tsend.at[k], recv_sem=trecv.at[k],
            device_id=(lax.rem(probe + k, probe_n), space), device_id_type=MESH,
        )

    spread((xb, xg, xy, cq))
    for k in range(1, probe_n):
        trace_copy(k).start()

    def fourth(p, carry):
        x = combine([scale(k, p) for k in range(4)], field(signs, p), split(g_own[p]), split(y_own[p]), split(q_own[p]))
        keep(x_own, p, x)
        return carry

    def out_copy(c):
        at = pl.ds(c * chunk, chunk)
        return pltpu.make_async_copy(x_own.at[at], out_hbm.at[at], out_sem.at[c])

    for c in range(chunks):
        lax.fori_loop(c * chunk, (c + 1) * chunk, fourth, 0)
        out_copy(c).start()

    for k in range(1, probe_n):
        trace_copy(k).wait_recv()
    tr_parts[0] = tr_mine[...]
    total = None
    for s in range(probe_n):
        part = tr_parts[lax.rem(probe - s + probe_n, probe_n)]
        total = part if total is None else total + part
    trace_ref[0, 0] = jnp.sum(total[0:1]) * (1.0 / float(probes * probe_n))

    for side, there in ((0, has_prev), (1, has_next)):
        @pl.when(there)
        def _():
            diag_copy(side).wait_send()
            for stage in (0, 1):
                for c in range(chunks):
                    halo_copy(stage, c, side).wait_send()
    for which in (0, 1):
        for k in range(1, space_n):
            sum_copy(which, k).wait_send()
    for k in range(1, probe_n):
        trace_copy(k).wait_send()
    for c in range(chunks):
        out_copy(c).wait()


def solution(mesh):
    probe_n, space_n = mesh.shape["probe"], mesh.shape["space"]

    def on_device(probe_signs, sensor_mask, sensor_weight, prior_mass):
        probes, rows, cols = probe_signs.shape
        chunk = next(c for c in (8, 6, 4, 3, 2, 1) if probes % c == 0)
        chunks = probes // chunk
        full = (probes, rows, cols)
        dma = pltpu.SemaphoreType.DMA
        vmem = pl.BlockSpec(memory_space=pltpu.VMEM)
        f32 = jnp.float32
        solved, trace = pl.pallas_call(
            functools.partial(kernel, ("probe", "space"), chunk),
            out_shape=(jax.ShapeDtypeStruct(full, f32), jax.ShapeDtypeStruct((1, 1), f32)),
            in_specs=[pl.BlockSpec(memory_space=pl.ANY), vmem, vmem, vmem],
            out_specs=(pl.BlockSpec(memory_space=pl.ANY), pl.BlockSpec(memory_space=pltpu.SMEM)),
            scratch_shapes=[
                pltpu.VMEM(full, jnp.int32), pltpu.VMEM(full, jnp.int32), pltpu.VMEM(full, jnp.int32),
                pltpu.VMEM((rows, cols), f32), pltpu.VMEM((rows, cols), f32),
                pltpu.VMEM(full, f32), pltpu.VMEM(full, f32), pltpu.VMEM(full, f32), pltpu.VMEM(full, f32),
                pltpu.VMEM(full, f32), pltpu.VMEM(full, f32),
                pltpu.VMEM((8, probes, LANES), f32),
                pltpu.VMEM((2, 8, LANES), f32), pltpu.VMEM((2, space_n, 8, LANES), f32),
                pltpu.VMEM((8, LANES), f32), pltpu.VMEM((probe_n, 8, LANES), f32),
                pltpu.VMEM((8, probes, LANES), f32),
                dma, dma((chunks,)), dma((2,)), dma((2,)),
                dma((2, 2, chunks)), dma((2, 2, chunks)),
                dma((2, space_n)), dma((2, space_n)), dma((probe_n,)), dma((probe_n,)),
            ],
            compiler_params=pltpu.CompilerParams(collective_id=0, has_side_effects=True),
            name="cg",
        )(probe_signs, sensor_mask, sensor_weight, prior_mass)
        return solved, trace.reshape(())

    return jax.shard_map(
        on_device,
        mesh=mesh,
        in_specs=(P("probe", "space", None), P("space", None), P("space", None), P("space", None)),
        out_specs=(P("probe", "space", None), P()),
        check_vma=False,
    )
```

```python
import functools

import jax
import jax.numpy as jnp
from jax import lax
from jax.experimental import pallas as pl
from jax.experimental.pallas import tpu as pltpu
from jax.sharding import PartitionSpec as P

MESH = pl.DeviceIdType.MESH
LANES = 128
SHIFT = 4.0
LOW = 0.02
TINY = 1e-30


def split(block):
    return [block[:, t * LANES : (t + 1) * LANES] for t in range(block.shape[1] // LANES)]


def sideways(tiles, lane):
    ahead = [pltpu.roll(v, 1, 1) for v in tiles]
    behind = [pltpu.roll(v, LANES - 1, 1) for v in tiles]
    zero = jnp.zeros_like(tiles[0])
    count = len(tiles)
    out = []
    for t in range(count):
        west = jnp.where(lane == 0, ahead[t - 1] if t else zero, ahead[t])
        east = jnp.where(lane == LANES - 1, behind[t + 1] if t + 1 < count else zero, behind[t])
        out.append(west + east)
    return out


def upright(own, halo, row, want_own, want_halo):
    rows = own[0].shape[0]
    for_own, for_halo = [], []
    for o, h in zip(own, halo):
        o_down, h_down = pltpu.roll(o, 1, 0), pltpu.roll(h, 1, 0)
        o_up, h_up = pltpu.roll(o, rows - 1, 0), pltpu.roll(h, rows - 1, 0)
        if want_own:
            for_own.append(jnp.where(row == 0, h_down, o_down) + jnp.where(row == rows - 1, h_up, o_up))
        if want_halo:
            for_halo.append(jnp.where(row == 0, o_down, h_down) + jnp.where(row == rows - 1, o_up, h_up))
    return for_own, for_halo


def apply_own(own, halo, diag, lane, row):
    up, _ = upright(own, halo, row, True, False)
    side = sideways(own, lane)
    return [d * v - (u + s) for d, v, u, s in zip(diag, own, up, side)]


def apply_halo(own, halo, diag, mask, lane, row):
    _, up = upright(own, halo, row, False, True)
    side = sideways(halo, lane)
    return [d * v - mask * (u + s) for d, v, u, s in zip(diag, halo, up, side)]


def apply_both(own, halo, diag, diag_h, mask, lane, row):
    up, up_h = upright(own, halo, row, True, True)
    side, side_h = sideways(own, lane), sideways(halo, lane)
    return (
        [d * v - (u + s) for d, v, u, s in zip(diag, own, up, side)],
        [d * v - mask * (u + s) for d, v, u, s in zip(diag_h, halo, up_h, side_h)],
    )


def dot(left, right):
    total = left[0] * right[0]
    for a, b in zip(left[1:], right[1:]):
        total = total + a * b
    return jnp.sum(total, axis=0, keepdims=True)


def first_steps(m1, m2, m3, m4):
    sigma = SHIFT
    a0 = sigma + m1
    b1 = jnp.maximum(m2 - m1 * m1, 0.0)
    h3 = m3 - 2.0 * m1 * m2 + m1 * m1 * m1
    s0 = 1.0 / jnp.maximum(a0, LOW)
    rr1 = s0 * s0 * b1
    pq1 = s0 * s0 * (h3 + sigma * b1) - rr1 * rr1 / s0
    s1 = rr1 / jnp.maximum(jnp.maximum(pq1, LOW * rr1), TINY)
    p1b, p1g = s0 * m1 + rr1, -s0
    r2b = s0 * m1 - s1 * sigma * p1b
    r2g = -s0 - s1 * (sigma * p1g + p1b)
    r2y = -s1 * p1g
    rr2 = jnp.maximum(r2y * (r2b * m2 + r2g * m3 + r2y * m4), 0.0)
    be1 = rr2 / jnp.maximum(rr1, TINY)
    p2b, p2g, p2y = r2b + be1 * p1b, r2g + be1 * p1g, r2y
    return dict(s0=s0, s1=s1, p1b=p1b, p1g=p1g, pq1=pq1, be1=be1, r2=(r2b, r2g, r2y), p2=(p2b, p2g, p2y))


def last_steps(st, sums):
    rr, rp, pp, pq, rq, qq, rw, qw = sums
    sigma = SHIFT
    full_pq = pq + sigma * pp
    s2 = rr / jnp.maximum(jnp.maximum(full_pq, LOW * rr), TINY)
    full_rq = rq + sigma * rp
    full_qq = qq + 2.0 * sigma * pq + sigma * sigma * pp
    rr3 = jnp.maximum(rr - 2.0 * s2 * full_rq + s2 * s2 * full_qq, 0.0)
    be2 = rr3 / jnp.maximum(rr, TINY)
    rhr2 = full_pq + st["be1"] * st["be1"] * st["pq1"]
    rhq = rw + 2.0 * sigma * rq + sigma * sigma * rp
    qhq = qw + 3.0 * sigma * qq + 3.0 * sigma * sigma * pq + sigma * sigma * sigma * pp
    rhr3 = rhr2 - 2.0 * s2 * rhq + s2 * s2 * qhq
    pq3 = rhr3 - rr3 * rr3 / jnp.maximum(rr * s2, TINY)
    s3 = rr3 / jnp.maximum(jnp.maximum(pq3, LOW * rr3), TINY)
    cp, cr, cq = s2 + s3 * (be2 - s2 * sigma), s3, -s3 * s2
    r2, p2 = st["r2"], st["p2"]
    xb = st["s0"] + st["s1"] * st["p1b"] + cp * p2[0] + cr * r2[0]
    xg = st["s1"] * st["p1g"] + cp * p2[1] + cr * r2[1]
    xy = cp * p2[2] + cr * r2[2]
    return xb, xg, xy, cq


def kernel(
    names, chunk, signs_hbm, mask_ref, weight_ref, prior_ref, x_own, trace_ref,
    signs, halo, halo_far, b_own, b_halo, diag, diag_h, g_own, g_halo, y_own, y_halo, q_own,
    acc, mine, parts, tr_mine, tr_parts, coef,
    load_sem, dsend, drecv, hsend, hrecv, ssend, srecv, tsend, trecv, space_in, probe_in,
):
    probe_axis, space_axis = names
    probe, space = lax.axis_index(probe_axis), lax.axis_index(space_axis)
    probe_n, space_n = lax.axis_size(probe_axis), lax.axis_size(space_axis)
    probes, rows, cols = signs.shape
    half = rows // 2
    quarter = half // 2
    chunks = probes // chunk
    cells = float(rows * space_n * cols)

    barrier = pltpu.get_barrier_semaphore()
    has_prev, has_next = space > 0, space < space_n - 1
    prev, nxt = (probe, jnp.maximum(space - 1, 0)), (probe, jnp.minimum(space + 1, space_n - 1))

    def meet(sem, distance):
        for there, other in (
            (space >= distance, jnp.maximum(space - distance, 0)),
            (space + distance < space_n, jnp.minimum(space + distance, space_n - 1)),
        ):
            @pl.when(there)
            def _():
                pl.semaphore_signal(sem, 1, device_id=(probe, other), device_id_type=MESH)

    def met(distance):
        return jnp.where(space >= distance, 1, 0) + jnp.where(space + distance < space_n, 1, 0)

    def flip(bit):
        size = 1 << bit
        return probe + size * (1 - 2 * lax.rem(probe // size, 2))

    probe_bits = (probe_n - 1).bit_length()
    space_bits = (space_n - 1).bit_length()
    meet(barrier, 1)
    for bit in range(probe_bits):
        pl.semaphore_signal(barrier, 1, device_id=(flip(bit), space), device_id_type=MESH)
    loads = pltpu.make_async_copy(signs_hbm, signs, load_sem)
    loads.start()
    diag[...] = mask_ref[...].astype(jnp.float32) * weight_ref[...] + prior_ref[...]
    loads.wait()
    pl.semaphore_wait(barrier, met(1) + probe_bits)

    def pieces(stage):
        if stage == 0:
            return (0, quarter), (rows - quarter, quarter)
        return (quarter, half - quarter), (half, half - quarter)

    def halo_copy(stage, c, side):
        start, size = pieces(stage)[side]
        at = (pl.ds(c * chunk, chunk), pl.ds(start, size))
        return pltpu.make_async_remote_copy(
            src_ref=signs.at[at], dst_ref=(halo, halo_far)[stage].at[at],
            send_sem=hsend.at[stage, side, c], recv_sem=hrecv.at[stage, side, c],
            device_id=(prev, nxt)[side], device_id_type=MESH,
        )

    def diag_copy(side):
        at = pl.ds(side * half, half)
        return pltpu.make_async_remote_copy(
            src_ref=diag.at[at], dst_ref=diag_h.at[at],
            send_sem=dsend.at[side], recv_sem=drecv.at[side],
            device_id=(prev, nxt)[side], device_id_type=MESH,
        )

    for side, there in ((0, has_prev), (1, has_next)):
        @pl.when(there)
        def _():
            diag_copy(side).start()
    for stage in (0, 1):
        for c in range(chunks):
            for side, there in ((0, has_prev), (1, has_next)):
                @pl.when(there)
                def _():
                    halo_copy(stage, c, side).start()

    for side, there in ((0, has_next), (1, has_prev)):
        @pl.when(there)
        def _():
            diag_copy(side).wait_recv()

    row = lax.broadcasted_iota(jnp.int32, (rows, LANES), 0)
    lane = lax.broadcasted_iota(jnp.int32, (rows, LANES), 1)
    below = jnp.where(has_next, 1.0, 0.0)
    above = jnp.where(has_prev, 1.0, 0.0)
    mask = jnp.where(row < half, below, above)
    live = mask > 0.5
    wide = lax.broadcasted_iota(jnp.int32, (rows, cols), 0)
    diag_h[...] = jnp.where(jnp.where(wide < half, below, above) > 0.5, diag_h[...], 0.0)

    def field(ref, p):
        return split(2.0 * ref[p].astype(jnp.float32) - 1.0)

    near = (row < quarter) | (row >= rows - quarter)

    def near_field(p):
        return [jnp.where(live & near, v, 0.0) for v in field(halo, p)]

    def halo_field(p):
        pairs = zip(split(halo[p]), split(halo_far[p]))
        return [jnp.where(live, 2.0 * jnp.where(near, a, b).astype(jnp.float32) - 1.0, 0.0) for a, b in pairs]

    def keep(ref, p, tiles):
        for t, v in enumerate(tiles):
            ref[p, :, t * LANES : (t + 1) * LANES] = v

    def first(p, carry):
        own, out = field(signs, p), near_field(p)
        d, dh = split(diag[...]), split(diag_h[...])
        g, gh = apply_both(own, out, d, dh, mask, lane, row)
        y = apply_own(g, gh, d, lane, row)
        keep(b_own, p, own)
        keep(g_own, p, g)
        keep(y_own, p, y)
        for k, (a, b) in enumerate(((own, g), (g, g), (g, y), (y, y))):
            acc[k, pl.ds(p, 1), :] = dot(a, b)
        return carry

    def second(p, carry):
        own, out = split(b_own[p]), halo_field(p)
        keep(b_halo, p, out)
        dh = split(diag_h[...])
        g = split(g_own[p])
        gh = apply_halo(own, out, dh, mask, lane, row)
        yh = apply_halo(g, gh, dh, mask, lane, row)
        keep(g_halo, p, gh)
        keep(y_halo, p, yh)
        return carry

    def await_halo(stage, c):
        for side, there in ((0, has_next), (1, has_prev)):
            @pl.when(there)
            def _():
                halo_copy(stage, c, side).wait_recv()

    def send_round(r):
        meet(space_in.at[r], 1 << r)
        for bit in range(probe_bits):
            if r < probe_bits - 1:
                pl.semaphore_signal(probe_in.at[r, bit], 1, device_id=(flip(bit), space), device_id_type=MESH)

    def end_round(r):
        pl.semaphore_wait(space_in.at[r], met(1 << r))
        for bit in range(probe_bits):
            if r < probe_bits - 1:
                pl.semaphore_wait(probe_in.at[r, bit], 1)

    rounds = max(space_bits, probe_bits - 1)
    for c in range(max(chunks, rounds + 1)):
        if 1 <= c <= rounds:
            end_round(c - 1)
        if c < rounds:
            send_round(c)
        if c < chunks:
            await_halo(0, c)
            lax.fori_loop(c * chunk, (c + 1) * chunk, first, 0)

    def sum_copy(which, k):
        other = lax.rem(space + k, space_n)
        return pltpu.make_async_remote_copy(
            src_ref=mine.at[which], dst_ref=parts.at[which, k],
            send_sem=ssend.at[which, k], recv_sem=srecv.at[which, k],
            device_id=(probe, other), device_id_type=MESH,
        )

    def send_sums(which, count):
        wide_lane = lax.broadcasted_iota(jnp.int32, (probes, LANES), 1)
        table = jnp.zeros((probes, LANES), jnp.float32)
        for k in range(count):
            table = jnp.where(wide_lane == k, jnp.sum(acc[k], axis=1, keepdims=True), table)
        table = jnp.concatenate([table, jnp.zeros((LANES - probes, LANES), jnp.float32)], axis=0)
        mine[which] = jnp.transpose(table)[:8]
        for k in range(1, space_n):
            sum_copy(which, k).start()

    def take_sums(which):
        for k in range(1, space_n):
            sum_copy(which, k).wait_recv()
        parts[which, 0] = mine[which]
        total = None
        for s in range(space_n):
            part = parts[which, lax.rem(space - s + space_n, space_n)]
            total = part if total is None else total + part
        total = total / cells
        return [total[k : k + 1] for k in range(8)]

    def spread(values):
        r8 = lax.broadcasted_iota(jnp.int32, (8, LANES), 0)
        table = jnp.zeros((8, LANES), jnp.float32)
        for k, v in enumerate(values):
            table = jnp.where(r8 == k, jnp.broadcast_to(v, (8, LANES)), table)
        table = jnp.concatenate([table, jnp.zeros((LANES - 8, LANES), jnp.float32)], axis=0)
        columns = jnp.transpose(table)
        for k in range(len(values)):
            coef[k] = jnp.broadcast_to(columns[:probes, k : k + 1], (probes, LANES))

    def combine(scales, *fields):
        out = []
        for tiles in zip(*fields):
            total = scales[0] * tiles[0]
            for s, v in zip(scales[1:], tiles[1:]):
                total = total + s * v
            out.append(total)
        return out

    def scale(k, p):
        return jnp.broadcast_to(coef[k, pl.ds(p, 1), :], (rows, LANES))

    send_sums(0, 4)
    for c in range(chunks):
        await_halo(1, c)
        lax.fori_loop(c * chunk, (c + 1) * chunk, second, 0)
    m1, m2, m3, m4 = take_sums(0)[:4]
    st = first_steps(m1, m2, m3, m4)
    spread(st["r2"] + st["p2"])

    def third(p, carry):
        own, out = split(b_own[p]), split(b_halo[p])
        g, y = split(g_own[p]), split(y_own[p])
        d, dh = split(diag[...]), split(diag_h[...])
        cs = [scale(k, p) for k in range(6)]
        p2 = combine(cs[3:], own, g, y)
        p2h = combine(cs[3:], out, split(g_halo[p]), split(y_halo[p]))
        q, qh = apply_both(p2, p2h, d, dh, mask, lane, row)
        keep(q_own, p, q)
        w = apply_own(q, qh, d, lane, row)
        r2 = combine(cs[:3], own, g, y)
        pairs = ((r2, r2), (r2, p2), (p2, p2), (p2, q), (r2, q), (q, q), (r2, w), (q, w))
        for k, (a, b) in enumerate(pairs):
            acc[k, pl.ds(p, 1), :] = dot(a, b)
        return carry

    lax.fori_loop(0, probes, third, 0)
    send_sums(1, 8)
    xb, xg, xy, cq = last_steps(st, take_sums(1))
    p2 = st["p2"]
    trace = xb + xg * m1 + xy * m2 + cq * (p2[0] * m1 + p2[1] * m2 + p2[2] * m3)
    lane1 = lax.broadcasted_iota(jnp.int32, (1, LANES), 1)
    trace = jnp.where(lane1 < probes, trace, 0.0)
    tr_mine[...] = jnp.broadcast_to(trace, tr_mine.shape)

    def trace_copy(k):
        return pltpu.make_async_remote_copy(
            src_ref=tr_mine, dst_ref=tr_parts.at[k],
            send_sem=tsend.at[k], recv_sem=trecv.at[k],
            device_id=(lax.rem(probe + k, probe_n), space), device_id_type=MESH,
        )

    spread((xb, xg, xy, cq))
    for k in range(1, probe_n):
        trace_copy(k).start()

    def fourth(p, carry):
        x = combine([scale(k, p) for k in range(4)], split(b_own[p]), split(g_own[p]), split(y_own[p]), split(q_own[p]))
        keep(x_own, p, x)
        return carry

    lax.fori_loop(0, probes, fourth, 0)

    for k in range(1, probe_n):
        trace_copy(k).wait_recv()
    tr_parts[0] = tr_mine[...]
    total = None
    for s in range(probe_n):
        part = tr_parts[lax.rem(probe - s + probe_n, probe_n)]
        total = part if total is None else total + part
    trace_ref[0, 0] = jnp.sum(total[0:1]) * (1.0 / float(probes * probe_n))

    for side, there in ((0, has_prev), (1, has_next)):
        @pl.when(there)
        def _():
            diag_copy(side).wait_send()
            for stage in (0, 1):
                for c in range(chunks):
                    halo_copy(stage, c, side).wait_send()
    for which in (0, 1):
        for k in range(1, space_n):
            sum_copy(which, k).wait_send()
    for k in range(1, probe_n):
        trace_copy(k).wait_send()


def solution(mesh):
    probe_n, space_n = mesh.shape["probe"], mesh.shape["space"]

    def on_device(probe_signs, sensor_mask, sensor_weight, prior_mass):
        probes, rows, cols = probe_signs.shape
        chunk = next(c for c in (8, 6, 4, 3, 2, 1) if probes % c == 0)
        chunks = probes // chunk
        full = (probes, rows, cols)
        dma, regular = pltpu.SemaphoreType.DMA, lambda n: pltpu.SemaphoreType.REGULAR(n)
        vmem = pl.BlockSpec(memory_space=pltpu.VMEM)
        f32 = jnp.float32
        solved, trace = pl.pallas_call(
            functools.partial(kernel, ("probe", "space"), chunk),
            out_shape=(pltpu.VMEM(full, f32), jax.ShapeDtypeStruct((1, 1), f32)),
            in_specs=[pl.BlockSpec(memory_space=pl.ANY), vmem, vmem, vmem],
            out_specs=(vmem, pl.BlockSpec(memory_space=pltpu.SMEM)),
            scratch_shapes=[
                pltpu.VMEM(full, jnp.int32), pltpu.VMEM(full, jnp.int32), pltpu.VMEM(full, jnp.int32),
                pltpu.VMEM(full, f32), pltpu.VMEM(full, f32),
                pltpu.VMEM((rows, cols), f32), pltpu.VMEM((rows, cols), f32),
                pltpu.VMEM(full, f32), pltpu.VMEM(full, f32), pltpu.VMEM(full, f32), pltpu.VMEM(full, f32),
                pltpu.VMEM(full, f32),
                pltpu.VMEM((8, probes, LANES), f32),
                pltpu.VMEM((2, 8, LANES), f32), pltpu.VMEM((2, space_n, 8, LANES), f32),
                pltpu.VMEM((8, LANES), f32), pltpu.VMEM((probe_n, 8, LANES), f32),
                pltpu.VMEM((8, probes, LANES), f32),
                dma, dma((2,)), dma((2,)),
                dma((2, 2, chunks)), dma((2, 2, chunks)),
                dma((2, space_n)), dma((2, space_n)), dma((probe_n,)), dma((probe_n,)),
                regular((8,)), regular((8, 8)),
            ],
            compiler_params=pltpu.CompilerParams(collective_id=0, has_side_effects=True),
            name="cg",
        )(probe_signs, sensor_mask, sensor_weight, prior_mass)
        return solved, trace.reshape(())

    return jax.shard_map(
        on_device,
        mesh=mesh,
        in_specs=(P("probe", "space", None), P("space", None), P("space", None), P("space", None)),
        out_specs=(P("probe", "space", None), P()),
        check_vma=False,
    )
```

```python
import functools

import jax
import jax.numpy as jnp
from jax import lax
from jax.experimental import pallas as pl
from jax.experimental.pallas import tpu as pltpu
from jax.sharding import PartitionSpec as P

MESH = pl.DeviceIdType.MESH
LANES = 128
SHIFT = 4.0
LOW = 0.02
TINY = 1e-30


def split(block):
    return [block[:, t * LANES : (t + 1) * LANES] for t in range(block.shape[1] // LANES)]


def sideways(tiles, lane):
    ahead = [pltpu.roll(v, 1, 1) for v in tiles]
    behind = [pltpu.roll(v, LANES - 1, 1) for v in tiles]
    zero = jnp.zeros_like(tiles[0])
    count = len(tiles)
    out = []
    for t in range(count):
        west = jnp.where(lane == 0, ahead[t - 1] if t else zero, ahead[t])
        east = jnp.where(lane == LANES - 1, behind[t + 1] if t + 1 < count else zero, behind[t])
        out.append(west + east)
    return out


def upright(own, halo, row, want_own, want_halo):
    rows = own[0].shape[0]
    for_own, for_halo = [], []
    for o, h in zip(own, halo):
        o_down, h_down = pltpu.roll(o, 1, 0), pltpu.roll(h, 1, 0)
        o_up, h_up = pltpu.roll(o, rows - 1, 0), pltpu.roll(h, rows - 1, 0)
        if want_own:
            for_own.append(jnp.where(row == 0, h_down, o_down) + jnp.where(row == rows - 1, h_up, o_up))
        if want_halo:
            for_halo.append(jnp.where(row == 0, o_down, h_down) + jnp.where(row == rows - 1, o_up, h_up))
    return for_own, for_halo


def apply_own(own, halo, diag, lane, row):
    up, _ = upright(own, halo, row, True, False)
    side = sideways(own, lane)
    return [d * v - (u + s) for d, v, u, s in zip(diag, own, up, side)]


def apply_halo(own, halo, diag, mask, lane, row):
    _, up = upright(own, halo, row, False, True)
    side = sideways(halo, lane)
    return [d * v - mask * (u + s) for d, v, u, s in zip(diag, halo, up, side)]


def apply_both(own, halo, diag, diag_h, mask, lane, row):
    up, up_h = upright(own, halo, row, True, True)
    side, side_h = sideways(own, lane), sideways(halo, lane)
    return (
        [d * v - (u + s) for d, v, u, s in zip(diag, own, up, side)],
        [d * v - mask * (u + s) for d, v, u, s in zip(diag_h, halo, up_h, side_h)],
    )


def dot(left, right):
    total = left[0] * right[0]
    for a, b in zip(left[1:], right[1:]):
        total = total + a * b
    return jnp.sum(total, axis=0, keepdims=True)


def first_steps(m1, m2, m3, m4):
    sigma = SHIFT
    a0 = sigma + m1
    b1 = jnp.maximum(m2 - m1 * m1, 0.0)
    h3 = m3 - 2.0 * m1 * m2 + m1 * m1 * m1
    s0 = 1.0 / jnp.maximum(a0, LOW)
    rr1 = s0 * s0 * b1
    pq1 = s0 * s0 * (h3 + sigma * b1) - rr1 * rr1 / s0
    s1 = rr1 / jnp.maximum(jnp.maximum(pq1, LOW * rr1), TINY)
    p1b, p1g = s0 * m1 + rr1, -s0
    r2b = s0 * m1 - s1 * sigma * p1b
    r2g = -s0 - s1 * (sigma * p1g + p1b)
    r2y = -s1 * p1g
    rr2 = jnp.maximum(r2y * (r2b * m2 + r2g * m3 + r2y * m4), 0.0)
    be1 = rr2 / jnp.maximum(rr1, TINY)
    p2b, p2g, p2y = r2b + be1 * p1b, r2g + be1 * p1g, r2y
    return dict(s0=s0, s1=s1, p1b=p1b, p1g=p1g, pq1=pq1, be1=be1, r2=(r2b, r2g, r2y), p2=(p2b, p2g, p2y))


def last_steps(st, sums):
    rr, rp, pp, pq, rq, qq, rw, qw = sums
    sigma = SHIFT
    full_pq = pq + sigma * pp
    s2 = rr / jnp.maximum(jnp.maximum(full_pq, LOW * rr), TINY)
    full_rq = rq + sigma * rp
    full_qq = qq + 2.0 * sigma * pq + sigma * sigma * pp
    rr3 = jnp.maximum(rr - 2.0 * s2 * full_rq + s2 * s2 * full_qq, 0.0)
    be2 = rr3 / jnp.maximum(rr, TINY)
    rhr2 = full_pq + st["be1"] * st["be1"] * st["pq1"]
    rhq = rw + 2.0 * sigma * rq + sigma * sigma * rp
    qhq = qw + 3.0 * sigma * qq + 3.0 * sigma * sigma * pq + sigma * sigma * sigma * pp
    rhr3 = rhr2 - 2.0 * s2 * rhq + s2 * s2 * qhq
    pq3 = rhr3 - rr3 * rr3 / jnp.maximum(rr * s2, TINY)
    s3 = rr3 / jnp.maximum(jnp.maximum(pq3, LOW * rr3), TINY)
    cp, cr, cq = s2 + s3 * (be2 - s2 * sigma), s3, -s3 * s2
    r2, p2 = st["r2"], st["p2"]
    xb = st["s0"] + st["s1"] * st["p1b"] + cp * p2[0] + cr * r2[0]
    xg = st["s1"] * st["p1g"] + cp * p2[1] + cr * r2[1]
    xy = cp * p2[2] + cr * r2[2]
    return xb, xg, xy, cq


def kernel(
    names, chunk, signs_hbm, mask_ref, weight_ref, prior_ref, x_own, trace_ref,
    signs, halo, halo_far, b_own, b_halo, diag, diag_h, g_own, g_halo, y_own, y_halo, q_own,
    acc, mine, parts, tr_mine, tr_parts, coef,
    load_sem, dsend, drecv, hsend, hrecv, ssend, srecv, tsend, trecv, space_in, probe_in,
):
    probe_axis, space_axis = names
    probe, space = lax.axis_index(probe_axis), lax.axis_index(space_axis)
    probe_n, space_n = lax.axis_size(probe_axis), lax.axis_size(space_axis)
    probes, rows, cols = signs.shape
    half = rows // 2
    quarter = half // 2
    chunks = probes // chunk
    cells = float(rows * space_n * cols)

    barrier = pltpu.get_barrier_semaphore()
    has_prev, has_next = space > 0, space < space_n - 1
    prev, nxt = (probe, jnp.maximum(space - 1, 0)), (probe, jnp.minimum(space + 1, space_n - 1))

    def meet(sem, distance):
        for there, other in (
            (space >= distance, jnp.maximum(space - distance, 0)),
            (space + distance < space_n, jnp.minimum(space + distance, space_n - 1)),
        ):
            @pl.when(there)
            def _():
                pl.semaphore_signal(sem, 1, device_id=(probe, other), device_id_type=MESH)

    def met(distance):
        return jnp.where(space >= distance, 1, 0) + jnp.where(space + distance < space_n, 1, 0)

    def flip(bit):
        size = 1 << bit
        return probe + size * (1 - 2 * lax.rem(probe // size, 2))

    probe_bits = (probe_n - 1).bit_length()
    space_bits = (space_n - 1).bit_length()
    meet(barrier, 1)
    for bit in range(probe_bits):
        pl.semaphore_signal(barrier, 1, device_id=(flip(bit), space), device_id_type=MESH)
    loads = pltpu.make_async_copy(signs_hbm, signs, load_sem)
    loads.start()
    diag[...] = mask_ref[...].astype(jnp.float32) * weight_ref[...] + prior_ref[...]
    loads.wait()
    pl.semaphore_wait(barrier, met(1) + probe_bits)

    def pieces(stage):
        if stage == 0:
            return (0, quarter), (rows - quarter, quarter)
        return (quarter, half - quarter), (half, half - quarter)

    def halo_copy(stage, c, side):
        start, size = pieces(stage)[side]
        at = (pl.ds(c * chunk, chunk), pl.ds(start, size))
        return pltpu.make_async_remote_copy(
            src_ref=signs.at[at], dst_ref=(halo, halo_far)[stage].at[at],
            send_sem=hsend.at[stage, side, c], recv_sem=hrecv.at[stage, side, c],
            device_id=(prev, nxt)[side], device_id_type=MESH,
        )

    def diag_copy(side):
        at = pl.ds(side * half, half)
        return pltpu.make_async_remote_copy(
            src_ref=diag.at[at], dst_ref=diag_h.at[at],
            send_sem=dsend.at[side], recv_sem=drecv.at[side],
            device_id=(prev, nxt)[side], device_id_type=MESH,
        )

    for side, there in ((0, has_prev), (1, has_next)):
        @pl.when(there)
        def _():
            diag_copy(side).start()
    for stage in (0, 1):
        for c in range(chunks):
            for side, there in ((0, has_prev), (1, has_next)):
                @pl.when(there)
                def _():
                    halo_copy(stage, c, side).start()

    for side, there in ((0, has_next), (1, has_prev)):
        @pl.when(there)
        def _():
            diag_copy(side).wait_recv()

    row = lax.broadcasted_iota(jnp.int32, (rows, LANES), 0)
    lane = lax.broadcasted_iota(jnp.int32, (rows, LANES), 1)
    below = jnp.where(has_next, 1.0, 0.0)
    above = jnp.where(has_prev, 1.0, 0.0)
    mask = jnp.where(row < half, below, above)
    live = mask > 0.5
    wide = lax.broadcasted_iota(jnp.int32, (rows, cols), 0)
    diag_h[...] = jnp.where(jnp.where(wide < half, below, above) > 0.5, diag_h[...], 0.0)

    def field(ref, p):
        return split(2.0 * ref[p].astype(jnp.float32) - 1.0)

    near = (row < quarter) | (row >= rows - quarter)

    def near_field(p):
        return [jnp.where(live & near, v, 0.0) for v in field(halo, p)]

    def halo_field(p):
        pairs = zip(split(halo[p]), split(halo_far[p]))
        return [jnp.where(live, 2.0 * jnp.where(near, a, b).astype(jnp.float32) - 1.0, 0.0) for a, b in pairs]

    def keep(ref, p, tiles):
        for t, v in enumerate(tiles):
            ref[p, :, t * LANES : (t + 1) * LANES] = v

    def first(p, carry):
        own, out = field(signs, p), near_field(p)
        d, dh = split(diag[...]), split(diag_h[...])
        g, gh = apply_both(own, out, d, dh, mask, lane, row)
        y = apply_own(g, gh, d, lane, row)
        keep(b_own, p, own)
        keep(g_own, p, g)
        keep(y_own, p, y)
        for k, (a, b) in enumerate(((own, g), (g, g), (g, y), (y, y))):
            acc[k, pl.ds(p, 1), :] = dot(a, b)
        return carry

    def second(p, carry):
        own, out = split(b_own[p]), halo_field(p)
        keep(b_halo, p, out)
        dh = split(diag_h[...])
        g = split(g_own[p])
        gh = apply_halo(own, out, dh, mask, lane, row)
        yh = apply_halo(g, gh, dh, mask, lane, row)
        keep(g_halo, p, gh)
        keep(y_halo, p, yh)
        return carry

    def await_halo(stage, c):
        for side, there in ((0, has_next), (1, has_prev)):
            @pl.when(there)
            def _():
                halo_copy(stage, c, side).wait_recv()

    def send_round(r):
        meet(space_in.at[r], 1 << r)
        for bit in range(probe_bits):
            if r < probe_bits - 1:
                pl.semaphore_signal(probe_in.at[r, bit], 1, device_id=(flip(bit), space), device_id_type=MESH)

    def end_round(r):
        pl.semaphore_wait(space_in.at[r], met(1 << r))
        for bit in range(probe_bits):
            if r < probe_bits - 1:
                pl.semaphore_wait(probe_in.at[r, bit], 1)

    rounds = max(space_bits, probe_bits - 1)
    for c in range(max(chunks, rounds + 1)):
        if 1 <= c <= rounds:
            end_round(c - 1)
        if c < rounds:
            send_round(c)
        if c < chunks:
            await_halo(0, c)
            lax.fori_loop(c * chunk, (c + 1) * chunk, first, 0, unroll=4)

    def sum_copy(which, k):
        other = lax.rem(space + k, space_n)
        return pltpu.make_async_remote_copy(
            src_ref=mine.at[which], dst_ref=parts.at[which, k],
            send_sem=ssend.at[which, k], recv_sem=srecv.at[which, k],
            device_id=(probe, other), device_id_type=MESH,
        )

    def send_sums(which, count):
        wide_lane = lax.broadcasted_iota(jnp.int32, (probes, LANES), 1)
        table = jnp.zeros((probes, LANES), jnp.float32)
        for k in range(count):
            table = jnp.where(wide_lane == k, jnp.sum(acc[k], axis=1, keepdims=True), table)
        table = jnp.concatenate([table, jnp.zeros((LANES - probes, LANES), jnp.float32)], axis=0)
        mine[which] = jnp.transpose(table)[:8]
        for k in range(1, space_n):
            sum_copy(which, k).start()

    def take_sums(which):
        for k in range(1, space_n):
            sum_copy(which, k).wait_recv()
        parts[which, 0] = mine[which]
        total = None
        for s in range(space_n):
            part = parts[which, lax.rem(space - s + space_n, space_n)]
            total = part if total is None else total + part
        total = total / cells
        return [total[k : k + 1] for k in range(8)]

    def spread(values):
        r8 = lax.broadcasted_iota(jnp.int32, (8, LANES), 0)
        table = jnp.zeros((8, LANES), jnp.float32)
        for k, v in enumerate(values):
            table = jnp.where(r8 == k, jnp.broadcast_to(v, (8, LANES)), table)
        table = jnp.concatenate([table, jnp.zeros((LANES - 8, LANES), jnp.float32)], axis=0)
        columns = jnp.transpose(table)
        for k in range(len(values)):
            coef[k] = jnp.broadcast_to(columns[:probes, k : k + 1], (probes, LANES))

    def combine(scales, *fields):
        out = []
        for tiles in zip(*fields):
            total = scales[0] * tiles[0]
            for s, v in zip(scales[1:], tiles[1:]):
                total = total + s * v
            out.append(total)
        return out

    def scale(k, p):
        return jnp.broadcast_to(coef[k, pl.ds(p, 1), :], (rows, LANES))

    send_sums(0, 4)
    for c in range(chunks):
        await_halo(1, c)
        lax.fori_loop(c * chunk, (c + 1) * chunk, second, 0, unroll=4)
    m1, m2, m3, m4 = take_sums(0)[:4]
    st = first_steps(m1, m2, m3, m4)
    spread(st["r2"] + st["p2"])

    def third(p, carry):
        own, out = split(b_own[p]), split(b_halo[p])
        g, y = split(g_own[p]), split(y_own[p])
        d, dh = split(diag[...]), split(diag_h[...])
        cs = [scale(k, p) for k in range(6)]
        p2 = combine(cs[3:], own, g, y)
        p2h = combine(cs[3:], out, split(g_halo[p]), split(y_halo[p]))
        q, qh = apply_both(p2, p2h, d, dh, mask, lane, row)
        keep(q_own, p, q)
        w = apply_own(q, qh, d, lane, row)
        r2 = combine(cs[:3], own, g, y)
        pairs = ((r2, r2), (r2, p2), (p2, p2), (p2, q), (r2, q), (q, q), (r2, w), (q, w))
        for k, (a, b) in enumerate(pairs):
            acc[k, pl.ds(p, 1), :] = dot(a, b)
        return carry

    lax.fori_loop(0, probes, third, 0, unroll=4)
    send_sums(1, 8)
    xb, xg, xy, cq = last_steps(st, take_sums(1))
    p2 = st["p2"]
    trace = xb + xg * m1 + xy * m2 + cq * (p2[0] * m1 + p2[1] * m2 + p2[2] * m3)
    lane1 = lax.broadcasted_iota(jnp.int32, (1, LANES), 1)
    trace = jnp.where(lane1 < probes, trace, 0.0)
    tr_mine[...] = jnp.broadcast_to(trace, tr_mine.shape)

    def trace_copy(k):
        return pltpu.make_async_remote_copy(
            src_ref=tr_mine, dst_ref=tr_parts.at[k],
            send_sem=tsend.at[k], recv_sem=trecv.at[k],
            device_id=(lax.rem(probe + k, probe_n), space), device_id_type=MESH,
        )

    for k in range(1, probe_n):
        trace_copy(k).start()
    spread((xb, xg, xy, cq))

    def fourth(p, carry):
        x = combine([scale(k, p) for k in range(4)], split(b_own[p]), split(g_own[p]), split(y_own[p]), split(q_own[p]))
        keep(x_own, p, x)
        return carry

    lax.fori_loop(0, probes, fourth, 0, unroll=4)

    for k in range(1, probe_n):
        trace_copy(k).wait_recv()
    tr_parts[0] = tr_mine[...]
    total = None
    for s in range(probe_n):
        part = tr_parts[lax.rem(probe - s + probe_n, probe_n)]
        total = part if total is None else total + part
    trace_ref[0, 0] = jnp.sum(total[0:1]) * (1.0 / float(probes * probe_n))

    for side, there in ((0, has_prev), (1, has_next)):
        @pl.when(there)
        def _():
            diag_copy(side).wait_send()
            for stage in (0, 1):
                for c in range(chunks):
                    halo_copy(stage, c, side).wait_send()
    for which in (0, 1):
        for k in range(1, space_n):
            sum_copy(which, k).wait_send()
    for k in range(1, probe_n):
        trace_copy(k).wait_send()


def solution(mesh):
    probe_n, space_n = mesh.shape["probe"], mesh.shape["space"]

    def on_device(probe_signs, sensor_mask, sensor_weight, prior_mass):
        probes, rows, cols = probe_signs.shape
        chunk = next(c for c in (8, 6, 4, 3, 2, 1) if probes % c == 0)
        chunks = probes // chunk
        full = (probes, rows, cols)
        dma, regular = pltpu.SemaphoreType.DMA, lambda n: pltpu.SemaphoreType.REGULAR(n)
        vmem = pl.BlockSpec(memory_space=pltpu.VMEM)
        f32 = jnp.float32
        solved, trace = pl.pallas_call(
            functools.partial(kernel, ("probe", "space"), chunk),
            out_shape=(pltpu.VMEM(full, f32), jax.ShapeDtypeStruct((1, 1), f32)),
            in_specs=[pl.BlockSpec(memory_space=pl.ANY), vmem, vmem, vmem],
            out_specs=(vmem, pl.BlockSpec(memory_space=pltpu.SMEM)),
            scratch_shapes=[
                pltpu.VMEM(full, jnp.int32), pltpu.VMEM(full, jnp.int32), pltpu.VMEM(full, jnp.int32),
                pltpu.VMEM(full, f32), pltpu.VMEM(full, f32),
                pltpu.VMEM((rows, cols), f32), pltpu.VMEM((rows, cols), f32),
                pltpu.VMEM(full, f32), pltpu.VMEM(full, f32), pltpu.VMEM(full, f32), pltpu.VMEM(full, f32),
                pltpu.VMEM(full, f32),
                pltpu.VMEM((8, probes, LANES), f32),
                pltpu.VMEM((2, 8, LANES), f32), pltpu.VMEM((2, space_n, 8, LANES), f32),
                pltpu.VMEM((8, LANES), f32), pltpu.VMEM((probe_n, 8, LANES), f32),
                pltpu.VMEM((8, probes, LANES), f32),
                dma, dma((2,)), dma((2,)),
                dma((2, 2, chunks)), dma((2, 2, chunks)),
                dma((2, space_n)), dma((2, space_n)), dma((probe_n,)), dma((probe_n,)),
                regular((8,)), regular((8, 8)),
            ],
            compiler_params=pltpu.CompilerParams(collective_id=0, has_side_effects=True),
            name="cg",
        )(probe_signs, sensor_mask, sensor_weight, prior_mass)
        return solved, trace.reshape(())

    return jax.shard_map(
        on_device,
        mesh=mesh,
        in_specs=(P("probe", "space", None), P("space", None), P("space", None), P("space", None)),
        out_specs=(P("probe", "space", None), P()),
        check_vma=False,
    )
```

```python
import functools

import jax
import jax.numpy as jnp
from jax import lax
from jax.experimental import pallas as pl
from jax.experimental.pallas import tpu as pltpu
from jax.sharding import PartitionSpec as P

MESH = pl.DeviceIdType.MESH
LANES = 128
SHIFT = 4.0
LOW = 0.02
TINY = 1e-30


def split(block):
    return [block[:, t * LANES : (t + 1) * LANES] for t in range(block.shape[1] // LANES)]


def sideways(tiles, lane):
    ahead = [pltpu.roll(v, 1, 1) for v in tiles]
    behind = [pltpu.roll(v, LANES - 1, 1) for v in tiles]
    zero = jnp.zeros_like(tiles[0])
    count = len(tiles)
    out = []
    for t in range(count):
        west = jnp.where(lane == 0, ahead[t - 1] if t else zero, ahead[t])
        east = jnp.where(lane == LANES - 1, behind[t + 1] if t + 1 < count else zero, behind[t])
        out.append(west + east)
    return out


def upright(own, halo, row, want_own, want_halo):
    rows = own[0].shape[0]
    for_own, for_halo = [], []
    for o, h in zip(own, halo):
        o_down, h_down = pltpu.roll(o, 1, 0), pltpu.roll(h, 1, 0)
        o_up, h_up = pltpu.roll(o, rows - 1, 0), pltpu.roll(h, rows - 1, 0)
        if want_own:
            for_own.append(jnp.where(row == 0, h_down, o_down) + jnp.where(row == rows - 1, h_up, o_up))
        if want_halo:
            for_halo.append(jnp.where(row == 0, o_down, h_down) + jnp.where(row == rows - 1, o_up, h_up))
    return for_own, for_halo


def apply_own(own, halo, diag, lane, row):
    up, _ = upright(own, halo, row, True, False)
    side = sideways(own, lane)
    return [d * v - (u + s) for d, v, u, s in zip(diag, own, up, side)]


def apply_halo(own, halo, diag, mask, lane, row):
    _, up = upright(own, halo, row, False, True)
    side = sideways(halo, lane)
    return [d * v - mask * (u + s) for d, v, u, s in zip(diag, halo, up, side)]


def apply_both(own, halo, diag, diag_h, mask, lane, row):
    up, up_h = upright(own, halo, row, True, True)
    side, side_h = sideways(own, lane), sideways(halo, lane)
    return (
        [d * v - (u + s) for d, v, u, s in zip(diag, own, up, side)],
        [d * v - mask * (u + s) for d, v, u, s in zip(diag_h, halo, up_h, side_h)],
    )


def dot(left, right):
    total = left[0] * right[0]
    for a, b in zip(left[1:], right[1:]):
        total = total + a * b
    return jnp.sum(total, axis=0, keepdims=True)


def first_steps(m1, m2, m3, m4):
    sigma = SHIFT
    a0 = sigma + m1
    b1 = jnp.maximum(m2 - m1 * m1, 0.0)
    h3 = m3 - 2.0 * m1 * m2 + m1 * m1 * m1
    s0 = 1.0 / jnp.maximum(a0, LOW)
    rr1 = s0 * s0 * b1
    pq1 = s0 * s0 * (h3 + sigma * b1) - rr1 * rr1 / s0
    s1 = rr1 / jnp.maximum(jnp.maximum(pq1, LOW * rr1), TINY)
    p1b, p1g = s0 * m1 + rr1, -s0
    r2b = s0 * m1 - s1 * sigma * p1b
    r2g = -s0 - s1 * (sigma * p1g + p1b)
    r2y = -s1 * p1g
    rr2 = jnp.maximum(r2y * (r2b * m2 + r2g * m3 + r2y * m4), 0.0)
    be1 = rr2 / jnp.maximum(rr1, TINY)
    p2b, p2g, p2y = r2b + be1 * p1b, r2g + be1 * p1g, r2y
    return dict(s0=s0, s1=s1, p1b=p1b, p1g=p1g, pq1=pq1, be1=be1, r2=(r2b, r2g, r2y), p2=(p2b, p2g, p2y))


def last_steps(st, sums):
    rr, rp, pp, pq, rq, qq, rw, qw = sums
    sigma = SHIFT
    full_pq = pq + sigma * pp
    s2 = rr / jnp.maximum(jnp.maximum(full_pq, LOW * rr), TINY)
    full_rq = rq + sigma * rp
    full_qq = qq + 2.0 * sigma * pq + sigma * sigma * pp
    rr3 = jnp.maximum(rr - 2.0 * s2 * full_rq + s2 * s2 * full_qq, 0.0)
    be2 = rr3 / jnp.maximum(rr, TINY)
    rhr2 = full_pq + st["be1"] * st["be1"] * st["pq1"]
    rhq = rw + 2.0 * sigma * rq + sigma * sigma * rp
    qhq = qw + 3.0 * sigma * qq + 3.0 * sigma * sigma * pq + sigma * sigma * sigma * pp
    rhr3 = rhr2 - 2.0 * s2 * rhq + s2 * s2 * qhq
    pq3 = rhr3 - rr3 * rr3 / jnp.maximum(rr * s2, TINY)
    s3 = rr3 / jnp.maximum(jnp.maximum(pq3, LOW * rr3), TINY)
    cp, cr, cq = s2 + s3 * (be2 - s2 * sigma), s3, -s3 * s2
    r2, p2 = st["r2"], st["p2"]
    xb = st["s0"] + st["s1"] * st["p1b"] + cp * p2[0] + cr * r2[0]
    xg = st["s1"] * st["p1g"] + cp * p2[1] + cr * r2[1]
    xy = cp * p2[2] + cr * r2[2]
    return xb, xg, xy, cq


def kernel(
    names, chunk, signs_hbm, mask_ref, weight_ref, prior_ref, x_own, trace_ref,
    signs, halo, halo_far, b_own, b_halo, diag, diag_h, g_own, g_halo, y_own, y_halo, q_own,
    acc, mine, parts, tr_mine, tr_parts, coef,
    load_sem, dsend, drecv, hsend, hrecv, ssend, srecv, tsend, trecv, space_in, probe_in,
):
    probe_axis, space_axis = names
    probe, space = lax.axis_index(probe_axis), lax.axis_index(space_axis)
    probe_n, space_n = lax.axis_size(probe_axis), lax.axis_size(space_axis)
    probes, rows, cols = signs.shape
    half = rows // 2
    quarter = half // 2
    chunks = probes // chunk
    cells = float(rows * space_n * cols)

    barrier = pltpu.get_barrier_semaphore()
    has_prev, has_next = space > 0, space < space_n - 1
    prev, nxt = (probe, jnp.maximum(space - 1, 0)), (probe, jnp.minimum(space + 1, space_n - 1))

    def meet(sem, distance):
        for there, other in (
            (space >= distance, jnp.maximum(space - distance, 0)),
            (space + distance < space_n, jnp.minimum(space + distance, space_n - 1)),
        ):
            @pl.when(there)
            def _():
                pl.semaphore_signal(sem, 1, device_id=(probe, other), device_id_type=MESH)

    def met(distance):
        return jnp.where(space >= distance, 1, 0) + jnp.where(space + distance < space_n, 1, 0)

    def flip(bit):
        size = 1 << bit
        return probe + size * (1 - 2 * lax.rem(probe // size, 2))

    probe_bits = (probe_n - 1).bit_length()
    space_bits = (space_n - 1).bit_length()
    meet(barrier, 1)
    for bit in range(probe_bits):
        pl.semaphore_signal(barrier, 1, device_id=(flip(bit), space), device_id_type=MESH)
    def load(c):
        at = pl.ds(c * chunk, chunk)
        return pltpu.make_async_copy(signs_hbm.at[at], signs.at[at], load_sem.at[c])

    for c in range(chunks):
        load(c).start()
    diag[...] = mask_ref[...].astype(jnp.float32) * weight_ref[...] + prior_ref[...]
    pl.semaphore_wait(barrier, met(1) + probe_bits)

    def pieces(stage):
        if stage == 0:
            return (0, quarter), (rows - quarter, quarter)
        return (quarter, half - quarter), (half, half - quarter)

    def halo_copy(stage, c, side):
        start, size = pieces(stage)[side]
        at = (pl.ds(c * chunk, chunk), pl.ds(start, size))
        return pltpu.make_async_remote_copy(
            src_ref=signs.at[at], dst_ref=(halo, halo_far)[stage].at[at],
            send_sem=hsend.at[stage, side, c], recv_sem=hrecv.at[stage, side, c],
            device_id=(prev, nxt)[side], device_id_type=MESH,
        )

    def diag_copy(side):
        at = pl.ds(side * half, half)
        return pltpu.make_async_remote_copy(
            src_ref=diag.at[at], dst_ref=diag_h.at[at],
            send_sem=dsend.at[side], recv_sem=drecv.at[side],
            device_id=(prev, nxt)[side], device_id_type=MESH,
        )

    for side, there in ((0, has_prev), (1, has_next)):
        @pl.when(there)
        def _():
            diag_copy(side).start()
    for stage in (0, 1):
        for c in range(chunks):
            if stage == 0:
                load(c).wait()
            for side, there in ((0, has_prev), (1, has_next)):
                @pl.when(there)
                def _():
                    halo_copy(stage, c, side).start()

    for side, there in ((0, has_next), (1, has_prev)):
        @pl.when(there)
        def _():
            diag_copy(side).wait_recv()

    row = lax.broadcasted_iota(jnp.int32, (rows, LANES), 0)
    lane = lax.broadcasted_iota(jnp.int32, (rows, LANES), 1)
    below = jnp.where(has_next, 1.0, 0.0)
    above = jnp.where(has_prev, 1.0, 0.0)
    mask = jnp.where(row < half, below, above)
    live = mask > 0.5
    wide = lax.broadcasted_iota(jnp.int32, (rows, cols), 0)
    diag_h[...] = jnp.where(jnp.where(wide < half, below, above) > 0.5, diag_h[...], 0.0)

    def field(ref, p):
        return split(2.0 * ref[p].astype(jnp.float32) - 1.0)

    near = (row < quarter) | (row >= rows - quarter)

    def near_field(p):
        return [jnp.where(live & near, v, 0.0) for v in field(halo, p)]

    def halo_field(p):
        pairs = zip(split(halo[p]), split(halo_far[p]))
        return [jnp.where(live, 2.0 * jnp.where(near, a, b).astype(jnp.float32) - 1.0, 0.0) for a, b in pairs]

    def keep(ref, p, tiles):
        for t, v in enumerate(tiles):
            ref[p, :, t * LANES : (t + 1) * LANES] = v

    def first(p, carry):
        own, out = field(signs, p), near_field(p)
        d, dh = split(diag[...]), split(diag_h[...])
        g, gh = apply_both(own, out, d, dh, mask, lane, row)
        y = apply_own(g, gh, d, lane, row)
        keep(b_own, p, own)
        keep(g_own, p, g)
        keep(y_own, p, y)
        for k, (a, b) in enumerate(((own, g), (g, g), (g, y), (y, y))):
            acc[k, pl.ds(p, 1), :] = dot(a, b)
        return carry

    def second(p, carry):
        own, out = split(b_own[p]), halo_field(p)
        keep(b_halo, p, out)
        dh = split(diag_h[...])
        g = split(g_own[p])
        gh = apply_halo(own, out, dh, mask, lane, row)
        yh = apply_halo(g, gh, dh, mask, lane, row)
        keep(g_halo, p, gh)
        keep(y_halo, p, yh)
        return carry

    def await_halo(stage, c):
        for side, there in ((0, has_next), (1, has_prev)):
            @pl.when(there)
            def _():
                halo_copy(stage, c, side).wait_recv()

    def send_round(r):
        meet(space_in.at[r], 1 << r)
        for bit in range(probe_bits):
            if r < probe_bits - 1:
                pl.semaphore_signal(probe_in.at[r, bit], 1, device_id=(flip(bit), space), device_id_type=MESH)

    def end_round(r):
        pl.semaphore_wait(space_in.at[r], met(1 << r))
        for bit in range(probe_bits):
            if r < probe_bits - 1:
                pl.semaphore_wait(probe_in.at[r, bit], 1)

    rounds = max(space_bits, probe_bits - 1)
    for c in range(max(chunks, rounds + 1)):
        if 1 <= c <= rounds:
            end_round(c - 1)
        if c < rounds:
            send_round(c)
        if c < chunks:
            await_halo(0, c)
            lax.fori_loop(c * chunk, (c + 1) * chunk, first, 0, unroll=4)

    def sum_copy(which, k):
        other = lax.rem(space + k, space_n)
        return pltpu.make_async_remote_copy(
            src_ref=mine.at[which], dst_ref=parts.at[which, k],
            send_sem=ssend.at[which, k], recv_sem=srecv.at[which, k],
            device_id=(probe, other), device_id_type=MESH,
        )

    def send_sums(which, count):
        wide_lane = lax.broadcasted_iota(jnp.int32, (probes, LANES), 1)
        table = jnp.zeros((probes, LANES), jnp.float32)
        for k in range(count):
            table = jnp.where(wide_lane == k, jnp.sum(acc[k], axis=1, keepdims=True), table)
        table = jnp.concatenate([table, jnp.zeros((LANES - probes, LANES), jnp.float32)], axis=0)
        mine[which] = jnp.transpose(table)[:8]
        for k in range(1, space_n):
            sum_copy(which, k).start()

    def take_sums(which):
        for k in range(1, space_n):
            sum_copy(which, k).wait_recv()
        parts[which, 0] = mine[which]
        total = None
        for s in range(space_n):
            part = parts[which, lax.rem(space - s + space_n, space_n)]
            total = part if total is None else total + part
        total = total / cells
        return [total[k : k + 1] for k in range(8)]

    def spread(values):
        r8 = lax.broadcasted_iota(jnp.int32, (8, LANES), 0)
        table = jnp.zeros((8, LANES), jnp.float32)
        for k, v in enumerate(values):
            table = jnp.where(r8 == k, jnp.broadcast_to(v, (8, LANES)), table)
        table = jnp.concatenate([table, jnp.zeros((LANES - 8, LANES), jnp.float32)], axis=0)
        columns = jnp.transpose(table)
        for k in range(len(values)):
            coef[k] = jnp.broadcast_to(columns[:probes, k : k + 1], (probes, LANES))

    def combine(scales, *fields):
        out = []
        for tiles in zip(*fields):
            total = scales[0] * tiles[0]
            for s, v in zip(scales[1:], tiles[1:]):
                total = total + s * v
            out.append(total)
        return out

    def scale(k, p):
        return jnp.broadcast_to(coef[k, pl.ds(p, 1), :], (rows, LANES))

    send_sums(0, 4)
    for c in range(chunks):
        await_halo(1, c)
        lax.fori_loop(c * chunk, (c + 1) * chunk, second, 0, unroll=4)
    m1, m2, m3, m4 = take_sums(0)[:4]
    st = first_steps(m1, m2, m3, m4)
    spread(st["r2"] + st["p2"])

    def third(p, carry):
        own, out = split(b_own[p]), split(b_halo[p])
        g, y = split(g_own[p]), split(y_own[p])
        d, dh = split(diag[...]), split(diag_h[...])
        cs = [scale(k, p) for k in range(6)]
        p2 = combine(cs[3:], own, g, y)
        p2h = combine(cs[3:], out, split(g_halo[p]), split(y_halo[p]))
        q, qh = apply_both(p2, p2h, d, dh, mask, lane, row)
        keep(q_own, p, q)
        w = apply_own(q, qh, d, lane, row)
        r2 = combine(cs[:3], own, g, y)
        pairs = ((r2, r2), (r2, p2), (p2, p2), (p2, q), (r2, q), (q, q), (r2, w), (q, w))
        for k, (a, b) in enumerate(pairs):
            acc[k, pl.ds(p, 1), :] = dot(a, b)
        return carry

    lax.fori_loop(0, probes, third, 0, unroll=4)
    send_sums(1, 8)
    xb, xg, xy, cq = last_steps(st, take_sums(1))
    p2 = st["p2"]
    trace = xb + xg * m1 + xy * m2 + cq * (p2[0] * m1 + p2[1] * m2 + p2[2] * m3)
    lane1 = lax.broadcasted_iota(jnp.int32, (1, LANES), 1)
    trace = jnp.where(lane1 < probes, trace, 0.0)
    tr_mine[...] = jnp.broadcast_to(trace, tr_mine.shape)

    def trace_copy(k):
        return pltpu.make_async_remote_copy(
            src_ref=tr_mine, dst_ref=tr_parts.at[k],
            send_sem=tsend.at[k], recv_sem=trecv.at[k],
            device_id=(lax.rem(probe + k, probe_n), space), device_id_type=MESH,
        )

    for k in range(1, probe_n):
        trace_copy(k).start()
    spread((xb, xg, xy, cq))

    def fourth(p, carry):
        x = combine([scale(k, p) for k in range(4)], split(b_own[p]), split(g_own[p]), split(y_own[p]), split(q_own[p]))
        keep(x_own, p, x)
        return carry

    lax.fori_loop(0, probes, fourth, 0, unroll=4)

    for k in range(1, probe_n):
        trace_copy(k).wait_recv()
    tr_parts[0] = tr_mine[...]
    total = None
    for s in range(probe_n):
        part = tr_parts[lax.rem(probe - s + probe_n, probe_n)]
        total = part if total is None else total + part
    trace_ref[0, 0] = jnp.sum(total[0:1]) * (1.0 / float(probes * probe_n))

    for side, there in ((0, has_prev), (1, has_next)):
        @pl.when(there)
        def _():
            diag_copy(side).wait_send()
            for stage in (0, 1):
                for c in range(chunks):
                    halo_copy(stage, c, side).wait_send()
    for which in (0, 1):
        for k in range(1, space_n):
            sum_copy(which, k).wait_send()
    for k in range(1, probe_n):
        trace_copy(k).wait_send()


def solution(mesh):
    probe_n, space_n = mesh.shape["probe"], mesh.shape["space"]

    def on_device(probe_signs, sensor_mask, sensor_weight, prior_mass):
        probes, rows, cols = probe_signs.shape
        chunk = next(c for c in (12, 8, 6, 4, 3, 2, 1) if probes % c == 0)
        chunks = probes // chunk
        full = (probes, rows, cols)
        dma, regular = pltpu.SemaphoreType.DMA, lambda n: pltpu.SemaphoreType.REGULAR(n)
        vmem = pl.BlockSpec(memory_space=pltpu.VMEM)
        f32 = jnp.float32
        solved, trace = pl.pallas_call(
            functools.partial(kernel, ("probe", "space"), chunk),
            out_shape=(pltpu.VMEM(full, f32), jax.ShapeDtypeStruct((1, 1), f32)),
            in_specs=[pl.BlockSpec(memory_space=pl.ANY), vmem, vmem, vmem],
            out_specs=(vmem, pl.BlockSpec(memory_space=pltpu.SMEM)),
            scratch_shapes=[
                pltpu.VMEM(full, jnp.int32), pltpu.VMEM(full, jnp.int32), pltpu.VMEM(full, jnp.int32),
                pltpu.VMEM(full, f32), pltpu.VMEM(full, f32),
                pltpu.VMEM((rows, cols), f32), pltpu.VMEM((rows, cols), f32),
                pltpu.VMEM(full, f32), pltpu.VMEM(full, f32), pltpu.VMEM(full, f32), pltpu.VMEM(full, f32),
                pltpu.VMEM(full, f32),
                pltpu.VMEM((8, probes, LANES), f32),
                pltpu.VMEM((2, 8, LANES), f32), pltpu.VMEM((2, space_n, 8, LANES), f32),
                pltpu.VMEM((8, LANES), f32), pltpu.VMEM((probe_n, 8, LANES), f32),
                pltpu.VMEM((8, probes, LANES), f32),
                dma((chunks,)), dma((2,)), dma((2,)),
                dma((2, 2, chunks)), dma((2, 2, chunks)),
                dma((2, space_n)), dma((2, space_n)), dma((probe_n,)), dma((probe_n,)),
                regular((8,)), regular((8, 8)),
            ],
            compiler_params=pltpu.CompilerParams(collective_id=0, has_side_effects=True),
            name="cg",
        )(probe_signs, sensor_mask, sensor_weight, prior_mass)
        return solved, trace.reshape(())

    return jax.shard_map(
        on_device,
        mesh=mesh,
        in_specs=(P("probe", "space", None), P("space", None), P("space", None), P("space", None)),
        out_specs=(P("probe", "space", None), P()),
        check_vma=False,
    )
```
